32 devices in a mesh: lon: 4 (over z), lat: 4 (over y, core), ens: 2 (over x).
Axes of the slice: x: 2, y: 2, z: 4, core: 2. Of those that a mesh axis runs over, the one named last changes fastest.
Arguments:
- inputs: bfloat16 [2, 4, 24, 96, 192], P('ens', None, 'lat', 'lon'), may hold values from -6 to 6
- cotangent: bfloat16 [2, 4, 24, 96, 192], P('ens', None, 'lat', 'lon'), may hold values from -6 to 6
- norm1_gain: float32 [192], replicated, may hold values from 0.25 to 1.75
- norm1_offset: float32 [192], replicated, may hold values from -1.5 to 1.5
- qkv_weight: float32 [192, 576], replicated, may hold values from -0.4375 to 0.4375
- qkv_bias: float32 [576], replicated, may hold values from -1.5 to 1.5
- bias_table: float32 [2, 4, 6, 12, 12, 23], P(None, 'lat'), may hold values from -4 to 302
- proj_weight: float32 [192, 192], replicated, may hold values from -0.4375 to 0.4375
- proj_bias: float32 [192], replicated, may hold values from -1.5 to 1.5
- norm2_gain: float32 [192], replicated, may hold values from 0.25 to 1.75
- norm2_offset: float32 [192], replicated, may hold values from -1.5 to 1.5
- fc1_weight: float32 [192, 768], replicated, may hold values from -0.4375 to 0.4375
- fc1_bias: float32 [768], replicated, may hold values from -1.5 to 1.5
- fc2_weight: float32 [768, 192], replicated, may hold values from -0.21875 to 0.21875
- fc2_bias: float32 [192], replicated, may hold values from -1.5 to 1.5
Outputs:
- block_out: bfloat16 [2, 4, 24, 96, 192], P('ens', None, 'lat', 'lon')
- input_grad: bfloat16 [2, 4, 24, 96, 192], P('ens', None, 'lat', 'lon')
- qkv_weight_grad: float32 [192, 576], P(None, 'lon')
- qkv_bias_grad: float32 [576], P('lon')
- proj_weight_grad: float32 [192, 192], P(None, 'lon')
- proj_bias_grad: float32 [192], P('lon')
- fc1_weight_grad: float32 [192, 768], P(None, 'lon')
- fc1_bias_grad: float32 [768], P('lon')
- fc2_weight_grad: float32 [768, 192], P(None, 'lon')
- fc2_bias_grad: float32 [192], P('lon')
- norm1_gain_grad: float32 [192], P('lon')
- norm1_offset_grad: float32 [192], P('lon')
- norm2_gain_grad: float32 [192], P('lon')
- norm2_offset_grad: float32 [192], P('lon')
- bias_table_grad: float32 [2, 4, 6, 12, 12, 23], P(None, 'lat')
The draws below stay inside these ranges and needn't reach their ends.
All inputs are finite; a program needn't handle non-finite values.
Results may differ from the reference program's by a relative error of at most 0.025.
Values may be sent and summed in bfloat16 or wider, within the bound.
A program may use at most 128 MiB of HBM per device.

```python
import math
import jax
import jax.numpy as jnp
from jax import lax

C = 192
HEADS = 6
FF = 768
WL = 2
WT = 6
WO = 12
LEV = 4
SHIFT = 6
MEMBERS = 2
NLAT = 24
NLON = 96
NWLAT = 4
TOKENS = 18432


def draw_bias_table(key, part):
    table_shape = (LEV // WL, NWLAT, HEADS, WL * WT, WL * WT, 2 * WO - 1)
    return jnp.clip(jax.random.normal(key, table_shape, jnp.float32), -4.0, 4.0)


def block_levels(key, shape, cuts, smallest, top_value):
    def one(axis_at, parts):
        draws = jax.random.uniform(jax.random.fold_in(jax.random.fold_in(key, 6), axis_at), (parts,), jnp.float32, smallest / len(cuts), top_value / len(cuts))
        return jnp.repeat(jnp.exp(draws), shape[axis_at] // parts).reshape((-1,) + (1,) * (len(shape) - axis_at - 1))

    loudness = one(*cuts[0])
    for cut in cuts[1:]:
        loudness = loudness * one(*cut)
    return loudness


def normal_values(own_key, shape, deviation, limit, shards=(), held_as=jnp.bfloat16):
    array = jax.random.normal(own_key, shape, jnp.float32) * deviation
    if len(shards) > 0:
        array = block_levels(own_key, shape, shards, -0.22, 0.18) * array
    return jnp.clip(array, min=-limit, max=limit).astype(held_as)


def setup_inputs(seed: int = 0) -> dict:
    key_list = jax.random.split(jax.random.key(seed), 16)
    return {
        "inputs": normal_values(key_list[0], (MEMBERS, LEV, NLAT, NLON, C), 1.0, 6.0, ((0, 2), (2, 4), (3, 4))),
        "cotangent": normal_values(key_list[1], (MEMBERS, LEV, NLAT, NLON, C), 1.0, 6.0, ((0, 2), (2, 4), (3, 4))),
        "norm1_gain": jnp.clip(1.0 + 0.15 * jax.random.normal(key_list[2], (C,), jnp.float32), 0.25, 1.75),
        "norm1_offset": normal_values(key_list[3], (C,), 0.3, 1.5, (), jnp.float32),
        "qkv_weight": normal_values(key_list[4], (C, 3 * C), C ** -0.5, 0.4375, (), jnp.float32),
        "qkv_bias": normal_values(key_list[5], (3 * C,), 0.3, 1.5, (), jnp.float32),
        "bias_table": draw_bias_table(jax.random.fold_in(key_list[15], 71), 0),
        "proj_weight": normal_values(key_list[7], (C, C), C ** -0.5, 0.4375, (), jnp.float32),
        "proj_bias": normal_values(key_list[8], (C,), 0.3, 1.5, (), jnp.float32),
        "norm2_gain": jnp.clip(1.0 + 0.15 * jax.random.normal(key_list[9], (C,), jnp.float32), 0.25, 1.75),
        "norm2_offset": normal_values(key_list[10], (C,), 0.3, 1.5, (), jnp.float32),
        "fc1_weight": normal_values(key_list[11], (C, FF), C ** -0.5, 0.4375, (), jnp.float32),
        "fc1_bias": normal_values(key_list[12], (FF,), 0.3, 1.5, (), jnp.float32),
        "fc2_weight": normal_values(key_list[13], (FF, C), FF ** -0.5, 0.21875, (), jnp.float32),
        "fc2_bias": normal_values(key_list[14], (C,), 0.3, 1.5, (), jnp.float32),
    }


EPS = 1e-05

def layer_norm(values, gain, offset):
    centre = lax.optimization_barrier(jnp.mean(values, axis=-1, keepdims=True))
    centred = values - centre
    spread = lax.optimization_barrier(jnp.mean(centred * centred, axis=-1, keepdims=True))
    return centred * lax.rsqrt(spread + EPS) * gain + offset

def gelu_tanh(values):
    return jax.nn.gelu(values, approximate=True)

def to_windows(field):
    members, levels, lat_rows, lon_cells, channels = field.shape
    shaped = field.reshape(members, levels // WL, WL, lat_rows // WT, WT, lon_cells // WO, WO, channels)
    shaped = shaped.transpose(0, 1, 3, 5, 2, 4, 6, 7)
    return shaped.reshape(members, levels // WL, lat_rows // WT, lon_cells // WO, WL * WT * WO, channels)

def from_windows(windows):
    members, level_wins, lat_wins, lon_wins, window_size, channels = windows.shape
    shaped = windows.reshape(members, level_wins, lat_wins, lon_wins, WL, WT, WO, channels)
    shaped = shaped.transpose(0, 1, 4, 2, 5, 3, 6, 7)
    return shaped.reshape(members, level_wins * WL, lat_wins * WT, lon_wins * WO, channels)

def offset_picker():
    grid_shape = (WO, WO, 2 * WO - 1)
    lag_index = lax.broadcasted_iota(jnp.int32, grid_shape, 0) - lax.broadcasted_iota(jnp.int32, grid_shape, 1) + (WO - 1)
    return (lag_index == lax.broadcasted_iota(jnp.int32, grid_shape, 2)).astype(jnp.float32)

def expand_bias(table_part, picker):
    level_wins, lat_wins, head_count = table_part.shape[:3]
    expanded = jnp.einsum('vahxyr,ijr->vahxiyj', table_part, picker, precision=lax.Precision.HIGHEST)
    window_size = WL * WT * WO
    return expanded.reshape(level_wins, lat_wins, head_count, window_size, window_size)

def shrink_bias(bias_grad, picker):
    level_wins, lat_wins, head_count = bias_grad.shape[:3]
    shaped = bias_grad.reshape(level_wins, lat_wins, head_count, WL * WT, WO, WL * WT, WO)
    return jnp.einsum('vahxiyj,ijr->vahxyr', shaped, picker, precision=lax.Precision.HIGHEST)

def attend(packed, bias_full, head_count):
    outer = packed.shape[:-1]
    feature_count = packed.shape[-1] // 3
    head_size = feature_count // head_count
    pieces = packed.reshape(outer + (3, head_count, head_size))
    query_rows = pieces[..., 0, :, :]
    key_rows = pieces[..., 1, :, :]
    value_rows = pieces[..., 2, :, :]
    scaling = head_size ** (-0.5)
    scores = jnp.einsum('mvawihd,mvawjhd->mvawhij', query_rows.astype(jnp.float32), key_rows.astype(jnp.float32)) * scaling
    scores = scores + bias_full[None, :, :, None]
    row_peak = lax.optimization_barrier(jnp.max(scores, axis=-1, keepdims=True))
    raised = jnp.exp(scores - row_peak)
    probabilities = raised / lax.optimization_barrier(jnp.sum(raised, axis=-1, keepdims=True))
    weights = probabilities.astype(jnp.bfloat16)
    mixture = jnp.einsum('mvawhij,mvawjhd->mvawihd', weights.astype(jnp.float32), value_rows.astype(jnp.float32)).astype(jnp.bfloat16)
    return (mixture.reshape(outer + (feature_count,)), (query_rows, key_rows, value_rows, probabilities, weights))

def attend_back(mixture_grad, saved_state, head_count):
    query_rows, key_rows, value_rows, probabilities, weights = saved_state
    outer = mixture_grad.shape[:-1]
    feature_count = mixture_grad.shape[-1]
    scaling = (feature_count // head_count) ** (-0.5)
    grad_heads = mixture_grad.reshape(query_rows.shape).astype(jnp.float32)
    prob_grad = jnp.einsum('mvawihd,mvawjhd->mvawhij', grad_heads, value_rows.astype(jnp.float32))
    value_grad = jnp.einsum('mvawhij,mvawihd->mvawjhd', weights.astype(jnp.float32), grad_heads).astype(jnp.bfloat16)
    score_grad = probabilities * (prob_grad - lax.optimization_barrier(jnp.sum(prob_grad * probabilities, axis=-1, keepdims=True)))
    score_low = score_grad.astype(jnp.bfloat16).astype(jnp.float32)
    query_grad = (jnp.einsum('mvawhij,mvawjhd->mvawihd', score_low, key_rows.astype(jnp.float32)) * scaling).astype(jnp.bfloat16)
    key_grad = (jnp.einsum('mvawhij,mvawihd->mvawjhd', score_low, query_rows.astype(jnp.float32)) * scaling).astype(jnp.bfloat16)
    packed_grad = jnp.stack([query_grad, key_grad, value_grad], axis=-3)
    return (packed_grad.reshape(outer + (3 * feature_count,)), score_grad)

def band_pass(inputs, cotangent, table_part, params):
    norm1_gain, norm1_offset, qkv_low, qkv_bias, proj_low, proj_bias, norm2_gain, norm2_offset, fc1_low, fc1_bias, fc2_low, fc2_bias = params
    channels = inputs.shape[-1]
    grid_shape = inputs.shape[:-1]
    inputs_wide = inputs.astype(jnp.float32)
    normed_wide, norm1_back = jax.vjp(layer_norm, inputs_wide, norm1_gain, norm1_offset)
    normed = normed_wide.astype(jnp.bfloat16)
    rolled = jnp.roll(normed, -SHIFT, axis=3)
    packed = jnp.dot(rolled.reshape(-1, channels), qkv_low, preferred_element_type=jnp.float32) + qkv_bias
    packed = to_windows(packed.astype(jnp.bfloat16).reshape(grid_shape + (3 * channels,)))
    picker = offset_picker()
    bias_full = expand_bias(table_part, picker)
    mixture, saved_state = attend(packed, bias_full, HEADS)
    attended = jnp.roll(from_windows(mixture), SHIFT, axis=3).reshape(-1, channels)
    attn_out = (jnp.dot(attended, proj_low, preferred_element_type=jnp.float32) + proj_bias).astype(jnp.bfloat16)
    resid = inputs_wide.reshape(-1, channels) + attn_out.astype(jnp.float32)
    normed2_wide, norm2_back = jax.vjp(layer_norm, resid, norm2_gain, norm2_offset)
    normed2 = normed2_wide.astype(jnp.bfloat16)
    pre_act = jnp.dot(normed2, fc1_low, preferred_element_type=jnp.float32) + fc1_bias
    activ_wide, gelu_back = jax.vjp(gelu_tanh, pre_act)
    activated = activ_wide.astype(jnp.bfloat16)
    block_out = (resid + jnp.dot(activated, fc2_low, preferred_element_type=jnp.float32) + fc2_bias).astype(jnp.bfloat16)
    cot_low = cotangent.reshape(-1, channels)
    cot_wide = cot_low.astype(jnp.float32)
    fc2_bias_grad = lax.optimization_barrier(jnp.sum(cot_wide, axis=0))
    fc2_weight_grad = jnp.dot(activated.T, cot_low, preferred_element_type=jnp.float32)
    act_grad = jnp.dot(cot_low, fc2_low.T, preferred_element_type=jnp.float32)
    pre_grad = gelu_back(act_grad)[0].astype(jnp.bfloat16)
    fc1_bias_grad = lax.optimization_barrier(jnp.sum(pre_grad.astype(jnp.float32), axis=0))
    fc1_weight_grad = jnp.dot(normed2.T, pre_grad, preferred_element_type=jnp.float32)
    normed2_grad = jnp.dot(pre_grad, fc1_low.T, preferred_element_type=jnp.float32)
    resid_part, norm2_gain_grad, norm2_offset_grad = norm2_back(normed2_grad)
    resid_grad = cot_wide + resid_part
    attn_grad = resid_grad.astype(jnp.bfloat16)
    proj_bias_grad = lax.optimization_barrier(jnp.sum(attn_grad.astype(jnp.float32), axis=0))
    proj_weight_grad = jnp.dot(attended.T, attn_grad, preferred_element_type=jnp.float32)
    attended_grad = jnp.dot(attn_grad, proj_low.T, preferred_element_type=jnp.float32).astype(jnp.bfloat16)
    rolled_grad = jnp.roll(attended_grad.reshape(grid_shape + (channels,)), -SHIFT, axis=3)
    packed_grad, score_grad = attend_back(to_windows(rolled_grad), saved_state, HEADS)
    table_grad = shrink_bias(lax.optimization_barrier(jnp.sum(score_grad, axis=(0, 3))), picker)
    qkv_grad = jnp.roll(from_windows(packed_grad), SHIFT, axis=3).reshape(-1, 3 * channels)
    qkv_bias_grad = lax.optimization_barrier(jnp.sum(qkv_grad.astype(jnp.float32), axis=0))
    qkv_weight_grad = jnp.dot(normed.reshape(-1, channels).T, qkv_grad, preferred_element_type=jnp.float32)
    normed_grad = jnp.dot(qkv_grad, qkv_low.T, preferred_element_type=jnp.float32)
    input_part, norm1_gain_grad, norm1_offset_grad = norm1_back(normed_grad.reshape(grid_shape + (channels,)))
    input_grad = (resid_grad.reshape(grid_shape + (channels,)) + input_part).astype(jnp.bfloat16)
    grads = (qkv_weight_grad, qkv_bias_grad, proj_weight_grad, proj_bias_grad, fc1_weight_grad, fc1_bias_grad, fc2_weight_grad, fc2_bias_grad, norm1_gain_grad, norm1_offset_grad, norm2_gain_grad, norm2_offset_grad)
    return (block_out.reshape(grid_shape + (channels,)), input_grad, grads, table_grad)

def reference(inputs, cotangent, norm1_gain, norm1_offset, qkv_weight, qkv_bias, bias_table, proj_weight, proj_bias, norm2_gain, norm2_offset, fc1_weight, fc1_bias, fc2_weight, fc2_bias):
    band_count = NLAT // WT
    params = (norm1_gain, norm1_offset, qkv_weight.astype(jnp.bfloat16), qkv_bias, proj_weight.astype(jnp.bfloat16), proj_bias, norm2_gain, norm2_offset, fc1_weight.astype(jnp.bfloat16), fc1_bias, fc2_weight.astype(jnp.bfloat16), fc2_bias)

    def to_bands(field):
        shaped = field.reshape(MEMBERS, LEV, band_count, WT, NLON, field.shape[-1])
        return jnp.moveaxis(shaped, 2, 0)

    def from_bands(stacked):
        return jnp.moveaxis(stacked, 0, 2).reshape(MEMBERS, LEV, NLAT, NLON, stacked.shape[-1])
    tables = jnp.moveaxis(bias_table, 1, 0)
    shapes = (qkv_weight, qkv_bias, proj_weight, proj_bias, fc1_weight, fc1_bias, fc2_weight, fc2_bias, norm1_gain, norm1_offset, norm2_gain, norm2_offset)
    initial = tuple((jnp.zeros(entry.shape, jnp.float32) for entry in shapes))

    def advance(carried, slices):
        inputs_band, cot_band, table_band = slices
        block_band, grad_band, grads, table_grad = band_pass(inputs_band, cot_band, table_band[:, None], params)
        summed = tuple((left + right for left, right in zip(carried, grads)))
        return (summed, (block_band, grad_band, table_grad[:, 0]))
    totals, (blocks, input_grads, table_grads) = lax.scan(advance, initial, (to_bands(inputs), to_bands(cotangent), tables))
    factor = 1.0 / math.sqrt(TOKENS)
    scaled = tuple((factor * entry for entry in totals))
    return (from_bands(blocks), from_bands(input_grads), scaled[0], scaled[1], scaled[2], scaled[3], scaled[4], scaled[5], scaled[6], scaled[7], scaled[8], scaled[9], scaled[10], scaled[11], jnp.moveaxis(table_grads, 0, 1))
```

```python
import functools
import math

import jax
import jax.numpy as jnp
from jax import lax
from jax.experimental import pallas as pl
from jax.experimental.pallas import tpu as pltpu
from jax.sharding import PartitionSpec as P

HEADS = 6
WL = 2
WT = 6
WO = 12
SHIFT = 6
GROUP = WL * WT
WIN = GROUP * WO
LAGS = 2 * WO - 1
EPS = 1e-05
F32 = jnp.float32
BF = jnp.bfloat16


def mm(a, b):
    return lax.dot_general(a, b, (((1,), (0,)), ((), ())), preferred_element_type=F32)


def mm_nt(a, b):
    return lax.dot_general(a, b, (((1,), (1,)), ((), ())), preferred_element_type=F32)


def mm_tn(a, b):
    return lax.dot_general(a, b, (((0,), (0,)), ((), ())), preferred_element_type=F32)


def ln_stats(values):
    centre = jnp.mean(values, axis=-1, keepdims=True)
    centred = values - centre
    spread = jnp.mean(centred * centred, axis=-1, keepdims=True)
    rstd = lax.rsqrt(spread + EPS)
    return centred * rstd, rstd


def ln_back(grad, gain, xhat, rstd):
    gx = grad * gain
    return rstd * (
        gx
        - jnp.mean(gx, axis=-1, keepdims=True)
        - xhat * jnp.mean(gx * xhat, axis=-1, keepdims=True)
    )


def lag_select(step, channels_in):
    cols = lax.broadcasted_iota(jnp.int32, (channels_in, WIN), 1)
    rows = lax.broadcasted_iota(jnp.int32, (channels_in, WIN), 0)
    want = (cols % GROUP) * LAGS - cols // GROUP + (WO - 1) + step
    return (rows == want).astype(F32).astype(BF)


def block_kernel(
    per_bias,
    factor,
    x_ref,
    cot_ref,
    g1_ref,
    b1_ref,
    wqkv_ref,
    bqkv_ref,
    table_ref,
    wproj_ref,
    bproj_ref,
    g2_ref,
    b2_ref,
    w1_ref,
    bf1_ref,
    w2_ref,
    bf2_ref,
    out_ref,
    gin_ref,
    gqkv_ref,
    gproj_ref,
    gfc1_ref,
    gfc2_ref,
    gtab_ref,
    bias,
    gsum,
    tab_rows,
    w1s,
    w2s,
    wqs,
    wks,
    wvs,
    wps,
    normed_s,
    norm2_s,
    att_s,
    agrad_s,
    pre_s,
    act_s,
    qg_s,
    kg_s,
    vg_s,
    aux_s,
    prob_s,
    low_s,
    qst_s,
    gst_s,
):
    channels = x_ref.shape[1]
    tokens = x_ref.shape[0]
    n_win = tokens // WIN
    n_bias = n_win // per_bias
    hd = channels // HEADS
    scaling = hd ** (-0.5)

    w1s[...] = w1_ref[...].astype(BF)
    w2s[...] = w2_ref[...].astype(BF)
    wps[...] = wproj_ref[...].astype(BF)
    wqs[...] = wqkv_ref[:, 0:channels].astype(BF)
    wks[...] = wqkv_ref[:, channels : 2 * channels].astype(BF)
    wvs[...] = wqkv_ref[:, 2 * channels : 3 * channels].astype(BF)

    table = table_ref[...]
    t1 = table.astype(BF)
    rest = table - t1.astype(F32)
    t2 = rest.astype(BF)
    t3 = (rest - t2.astype(F32)).astype(BF)
    for step in range(WO):
        sel = lag_select(step, table.shape[1])
        tab_rows[...] = mm(t1, sel) + mm(t2, sel) + mm(t3, sel)
        for n in range(n_bias):
            for h in range(HEADS):
                row = (n * HEADS + h) * GROUP
                bias[n, h * WIN + step * GROUP : h * WIN + (step + 1) * GROUP, :] = tab_rows[
                    row : row + GROUP, :
                ]
    gsum[...] = jnp.zeros_like(gsum)

    lane = lax.broadcasted_iota(jnp.int32, (WIN, channels), 1)

    def head(value, h):
        return jnp.where((lane >= h * hd) & (lane < (h + 1) * hd), value, jnp.zeros_like(value))

    def window(w, carry):
        rows = pl.ds(pl.multiple_of(w * WIN, WIN), WIN)
        nb = w // per_bias
        x = x_ref[rows, :].astype(F32)
        xhat1, rstd1 = ln_stats(x)
        normed = (xhat1 * g1_ref[...] + b1_ref[...]).astype(BF)
        normed_s[rows, :channels] = normed
        q = (mm(normed, wqs[...]) + bqkv_ref[:, 0:channels]).astype(BF)
        k = (mm(normed, wks[...]) + bqkv_ref[:, channels : 2 * channels]).astype(BF)
        v = (mm(normed, wvs[...]) + bqkv_ref[:, 2 * channels : 3 * channels]).astype(BF)
        mix = jnp.zeros((WIN, channels), F32)
        for h in range(HEADS):
            part = slice(h * WIN, (h + 1) * WIN)
            qh = head(q, h)
            qst_s[part, :] = qh
            s = mm_nt(qh, k) * scaling + bias[nb, part, :]
            e = jnp.exp(s - jnp.max(s, axis=-1, keepdims=True))
            p = e / jnp.sum(e, axis=-1, keepdims=True)
            prob_s[part, :] = p
            mix = mix + mm(p.astype(BF), head(v, h))
        att = mix.astype(BF)
        att_s[rows, :channels] = att
        attn_out = (mm(att, wps[...]) + bproj_ref[...]).astype(BF)
        resid = x + attn_out.astype(F32)
        xhat2, rstd2 = ln_stats(resid)
        normed2 = (xhat2 * g2_ref[...] + b2_ref[...]).astype(BF)
        norm2_s[rows, :channels] = normed2
        cot_low = cot_ref[rows, :]
        cot = cot_low.astype(F32)
        u = mm(normed2, w1s[...]) + bf1_ref[...]
        c0 = math.sqrt(2.0 / math.pi)
        usq = u * u
        t = jnp.tanh(c0 * u * (1.0 + 0.044715 * usq))
        half = 0.5 * (1.0 + t)
        act = (u * half).astype(BF)
        act_s[rows, : act.shape[1]] = act
        slope = half + 0.5 * u * (1.0 - t * t) * (c0 * (1.0 + (3 * 0.044715) * usq))
        out_ref[rows, :] = (resid + mm(act, w2s[...]) + bf2_ref[...]).astype(BF)
        pre = (mm_nt(cot_low, w2s[...]) * slope).astype(BF)
        pre_s[rows, :] = pre
        n2g = mm_nt(pre, w1s[...])
        rg = cot + ln_back(n2g, g2_ref[...], xhat2, rstd2)
        ag = rg.astype(BF)
        agrad_s[rows, :] = ag
        atg = mm_nt(ag, wps[...]).astype(BF)
        qg = jnp.zeros((WIN, channels), F32)
        for h in range(HEADS):
            part = slice(h * WIN, (h + 1) * WIN)
            gh = head(atg, h)
            gst_s[part, :] = gh
            p = prob_s[part, :]
            pg = mm_nt(gh, v)
            sg = p * (pg - jnp.sum(p * pg, axis=-1, keepdims=True))
            gsum[nb, part, :] += sg
            low = sg.astype(BF)
            low_s[part, :] = low
            qg = qg + mm(low, head(k, h))
        vg = mm_tn(prob_s[...].astype(BF), gst_s[...]).astype(BF)
        kg = (mm_tn(low_s[...], qst_s[...]) * scaling).astype(BF)
        qg = (qg * scaling).astype(BF)
        qg_s[rows, :] = qg
        kg_s[rows, :] = kg
        vg_s[rows, :] = vg
        ng = mm_nt(qg, wqs[...]) + mm_nt(kg, wks[...]) + mm_nt(vg, wvs[...])
        gin_ref[rows, :] = (rg + ln_back(ng, g1_ref[...], xhat1, rstd1)).astype(BF)
        sums = (
            jnp.sum(cot, axis=0, keepdims=True),
            jnp.sum(ag.astype(F32), axis=0, keepdims=True),
            jnp.sum(ng * xhat1, axis=0, keepdims=True),
            jnp.sum(ng, axis=0, keepdims=True),
            jnp.sum(n2g * xhat2, axis=0, keepdims=True),
            jnp.sum(n2g, axis=0, keepdims=True),
        )
        for i, total in enumerate(sums):
            aux_s[i : i + 1, :] += total
        return carry

    aux_s[...] = jnp.zeros_like(aux_s)
    ones = (lax.broadcasted_iota(jnp.int32, (tokens, 256 - channels), 1) == 0).astype(F32).astype(BF)
    normed_s[:, channels:] = ones
    norm2_s[:, channels:] = ones
    att_s[:, channels:] = jnp.zeros_like(ones)
    lax.fori_loop(0, n_win, window, 0)

    for i, ref in enumerate((qg_s, kg_s, vg_s)):
        gqkv_ref[i * channels : (i + 1) * channels, :] = (
            mm_tn(ref[...], normed_s[...]) * factor
        ).astype(BF)
    gfc1_ref[...] = (mm_tn(pre_s[...], norm2_s[...]) * factor).astype(BF)
    gfc2_ref[...] = (mm_tn(cot_ref[...], act_s[...]) * factor).astype(BF)
    wide = mm_tn(agrad_s[...], att_s[...])
    aux = jnp.transpose(aux_s[...])
    gproj_ref[:, :channels] = (wide[:, :channels] * factor).astype(BF)
    gproj_ref[:, channels : channels + 8] = (aux * factor).astype(BF)
    gproj_ref[:, channels + 8 :] = jnp.zeros_like(gproj_ref[:, channels + 8 :])

    total = jnp.zeros(table_ref.shape, F32)
    for step in range(WO):
        for n in range(n_bias):
            for h in range(HEADS):
                row = (n * HEADS + h) * GROUP
                tab_rows[row : row + GROUP, :] = gsum[
                    n, h * WIN + step * GROUP : h * WIN + (step + 1) * GROUP, :
                ]
        part = tab_rows[...]
        hi = part.astype(BF)
        lo = (part - hi.astype(F32)).astype(BF)
        sel = lag_select(step, table_ref.shape[1])
        total = total + mm_nt(hi, sel) + mm_nt(lo, sel)
    gtab_ref[...] = total.astype(BF)


def passed_along(value, axis, steps):
    count = lax.axis_size(axis)
    pairs = [(source, (source + steps) % count) for source in range(count)]
    return lax.ppermute(value, axis, pairs)


def widen(field):
    incoming = passed_along(field[..., :SHIFT, :], "lon", -1)
    return jnp.concatenate([field[..., SHIFT:, :], incoming], axis=-2)


def narrow(extended):
    cells = extended.shape[-2]
    returned = passed_along(extended[..., cells - SHIFT :, :], "lon", 1)
    return jnp.concatenate([returned, extended[..., : cells - SHIFT, :]], axis=-2)


def on_device(
    inputs,
    cotangent,
    norm1_gain,
    norm1_offset,
    qkv_weight,
    qkv_bias,
    bias_table,
    proj_weight,
    proj_bias,
    norm2_gain,
    norm2_offset,
    fc1_weight,
    fc1_bias,
    fc2_weight,
    fc2_bias,
):
    m, lev, lat, lon, c = inputs.shape
    v, a, o = lev // WL, lat // WT, lon // WO
    ff = fc1_weight.shape[1]
    tokens = m * lev * lat * lon
    nlon = lax.axis_size("lon")
    shards = nlon * lax.axis_size("lat") * lax.axis_size("ens")
    factor = 1.0 / math.sqrt(tokens * shards)
    both = widen(jnp.stack([inputs, cotangent]))
    both = both.reshape(2, m, v, WL, a, WT, o, WO, c)
    both = both.transpose(0, 2, 4, 1, 6, 7, 3, 5, 8).reshape(2, tokens, c)
    table2 = bias_table.reshape(v * a * HEADS * GROUP, GROUP * LAGS)

    sds = jax.ShapeDtypeStruct
    n_bias = v * a
    row = lambda vec: vec.reshape(1, -1)
    outs = pl.pallas_call(
        functools.partial(block_kernel, m * o, factor),
        out_shape=(
            sds((tokens, c), BF),
            sds((tokens, c), BF),
            sds((3 * c, 256), BF),
            sds((c, 256), BF),
            sds((ff, 256), BF),
            sds((c, ff), BF),
            sds(table2.shape, BF),
        ),
        in_specs=[pl.BlockSpec(memory_space=pltpu.VMEM)] * 15,
        out_specs=[pl.BlockSpec(memory_space=pltpu.VMEM)] * 7,
        scratch_shapes=[
            pltpu.VMEM((n_bias, HEADS * WIN, WIN), F32),
            pltpu.VMEM((n_bias, HEADS * WIN, WIN), F32),
            pltpu.VMEM((table2.shape[0], WIN), F32),
            pltpu.VMEM((c, ff), BF),
            pltpu.VMEM((ff, c), BF),
            pltpu.VMEM((c, c), BF),
            pltpu.VMEM((c, c), BF),
            pltpu.VMEM((c, c), BF),
            pltpu.VMEM((c, c), BF),
            pltpu.VMEM((tokens, 256), BF),
            pltpu.VMEM((tokens, 256), BF),
            pltpu.VMEM((tokens, 256), BF),
            pltpu.VMEM((tokens, c), BF),
            pltpu.VMEM((tokens, ff), BF),
            pltpu.VMEM((tokens, ff), BF),
            pltpu.VMEM((tokens, c), BF),
            pltpu.VMEM((tokens, c), BF),
            pltpu.VMEM((tokens, c), BF),
            pltpu.VMEM((8, c), F32),
            pltpu.VMEM((HEADS * WIN, WIN), F32),
            pltpu.VMEM((HEADS * WIN, WIN), BF),
            pltpu.VMEM((HEADS * WIN, c), BF),
            pltpu.VMEM((HEADS * WIN, c), BF),
        ],
        compiler_params=pltpu.CompilerParams(vmem_limit_bytes=56 * 1024 * 1024),
        cost_estimate=pl.CostEstimate(
            flops=4 * 10**9, bytes_accessed=8 * 10**6, transcendentals=10**6
        ),
    )(
        both[0],
        both[1],
        row(norm1_gain),
        row(norm1_offset),
        qkv_weight,
        row(qkv_bias),
        table2,
        proj_weight,
        row(proj_bias),
        row(norm2_gain),
        row(norm2_offset),
        fc1_weight,
        row(fc1_bias),
        fc2_weight,
        row(fc2_bias),
    )
    block_ext, gin_ext, gqkv, gproj, gfc1, gfc2, gtab = outs
    pair = jnp.stack([block_ext, gin_ext])
    pair = pair.reshape(2, v, a, m, o, WO, WL, WT, c).transpose(0, 3, 1, 6, 2, 7, 4, 5, 8)
    pair = narrow(pair.reshape(2, m, lev, lat, lon, c))

    packed = jnp.concatenate(
        [
            gqkv.reshape(nlon, -1, 256),
            gproj.reshape(nlon, -1, 256),
            gfc1.reshape(nlon, -1, 256),
            gfc2.reshape(nlon, -1, 256),
        ],
        axis=1,
    )
    share = lax.psum_scatter(packed, "lon", scatter_dimension=0, tiled=False)
    share = lax.psum(share, ("lat", "ens")).astype(F32)
    table_grad = lax.psum(gtab, ("lon", "ens")).astype(F32)
    n1, n2, n3, n4 = 3 * c // nlon, c // nlon, ff // nlon, c // nlon
    s_qkv, s_proj, s_fc1, s_fc2 = jnp.split(share, [n1, n1 + n2, n1 + n2 + n3], axis=0)
    s_fc2 = s_fc2.reshape(n4, ff)
    return (
        pair[0],
        pair[1],
        s_qkv[:, :c].T,
        s_qkv[:, c],
        s_proj[:, :c].T,
        s_proj[:, c + 1],
        s_fc1[:, :c].T,
        s_fc1[:, c],
        s_fc2.T,
        s_proj[:, c],
        s_proj[:, c + 2],
        s_proj[:, c + 3],
        s_proj[:, c + 4],
        s_proj[:, c + 5],
        table_grad.reshape(bias_table.shape),
    )


def solution(mesh):
    return jax.shard_map(
        on_device,
        mesh=mesh,
        in_specs=(
            P("ens", None, "lat", "lon", None),
            P("ens", None, "lat", "lon", None),
            P(),
            P(),
            P(),
            P(),
            P(None, "lat", None, None, None, None),
            P(),
            P(),
            P(),
            P(),
            P(),
            P(),
            P(),
            P(),
        ),
        out_specs=(
            P("ens", None, "lat", "lon", None),
            P("ens", None, "lat", "lon", None),
            P(None, "lon"),
            P("lon"),
            P(None, "lon"),
            P("lon"),
            P(None, "lon"),
            P("lon"),
            P(None, "lon"),
            P("lon"),
            P("lon"),
            P("lon"),
            P("lon"),
            P("lon"),
            P(None, "lat", None, None, None, None),
        ),
        check_vma=False,
    )
```
